32 devices in a mesh: rep: 2 (over z, core), dp: 16 (over x, y).
Axes of the slice: x: 4, y: 4, z: 1, core: 2. Of those that a mesh axis runs over, the one named last changes fastest.
The devices are a block of a 4x4x8 slice.
Arguments:
- x: bfloat16 [32, 1024, 512], P(('rep', 'dp')), parts along dimension 0
- dy: bfloat16 [32, 1024, 512], P(('rep', 'dp')), parts along dimension 0
- w_gate: bfloat16 [2, 512, 8192], P(None, 'dp')
- w_up: bfloat16 [2, 512, 8192], P(None, 'dp')
- w_down: bfloat16 [2, 8192, 512], P(None, 'dp')
Outputs:
- output 1: bfloat16 [32, 1024, 512], P(('rep', 'dp')), parts along dimension 0
- output 2: bfloat16 [4, 512, 8192], P('rep', 'dp'), parts along dimension 0
- output 3: bfloat16 [4, 512, 8192], P('rep', 'dp'), parts along dimension 0
- output 4: bfloat16 [4, 8192, 512], P('rep', 'dp'), parts along dimension 0
There are 2 independent parts. The reference program is written for one: setup_inputs(seed, part) draws one part's arguments, and reference() takes and returns one part's arrays. A program takes and returns all parts, laid end to end along the dimension named above; an argument that names none is the same for every part.
All inputs are finite; a program needn't handle non-finite values.
Results may differ from the reference program's by a relative error of at most 0.018.
Values are sent between devices in bfloat16 or wider.
A program may use at most 768 MiB of HBM per device.

```python
import jax
import jax.numpy as jnp
from jax import lax

SEQUENCES = 16
TOKENS = 1024
D = 512
FF = 8192
LAYERS = 2
NAMES = ("w_gate", "w_up", "w_down")
SHAPES = {"w_gate": (LAYERS, D, FF), "w_up": (LAYERS, D, FF), "w_down": (LAYERS, FF, D)}


def bump(key, n, height):
    away = (jnp.arange(n, dtype=jnp.int32) - jax.random.randint(key, (), 0, n, jnp.int32)) % n
    return jnp.where(away < n // 8, height, 1.0)


def together(key, own, strength):
    shared = jax.random.normal(key, own.shape[1:], jnp.float32)
    return (own + strength * shared) * lax.rsqrt(1 + strength * strength)


def setup_inputs(seed: int = 0, part: int = 0) -> dict:
    kx, kdy, ka, kb, kz, kf, kh, kl, *kw = jax.random.split(jax.random.key(seed), 8 + len(NAMES))
    kx, kdy, ka, kb = (jax.random.fold_in(k, part) for k in (kx, kdy, ka, kb))
    shape = (SEQUENCES, TOKENS, D)
    much_x, much_dy = jax.random.uniform(kz, (2,), jnp.float32, 0.0, 1.0)
    layers = 2.0 ** jax.random.uniform(kl, (LAYERS, 1, 1), jnp.float32, -1.0, 1.0)
    x = together(ka, jax.random.normal(kx, shape, jnp.float32), much_x) * bump(kf, D, 4.0)
    dy = together(kb, jax.random.normal(kdy, shape, jnp.float32), much_dy)
    drawn = {"x": x.astype(jnp.bfloat16), "dy": (dy * (SEQUENCES * TOKENS) ** -0.5).astype(jnp.bfloat16)}
    for key, name in zip(kw, NAMES, strict=True):
        w = jax.random.normal(key, SHAPES[name], jnp.float32) * SHAPES[name][1] ** -0.5
        drawn[name] = (w * {"w_gate": 1.0, "w_up": bump(kh, FF, 4.0), "w_down": layers}[name]).astype(jnp.bfloat16)
    return drawn


def matmul(a, w):
    return jnp.dot(a, w, preferred_element_type=jnp.float32).astype(jnp.bfloat16)


def normed(h):
    wide = h.astype(jnp.float32)
    scale = lax.rsqrt(jnp.mean(wide**2, -1, keepdims=True) + 1e-6)
    return (wide * scale).astype(jnp.bfloat16)


def layer(h, w):
    a = normed(h)
    gate = jnp.dot(a, w["w_gate"], preferred_element_type=jnp.float32)
    up = jnp.dot(a, w["w_up"], preferred_element_type=jnp.float32)
    return h + matmul((jax.nn.silu(gate) * up).astype(jnp.bfloat16), w["w_down"])


def stack(weights, h):
    return lax.scan(lambda h, w: (layer(h, w), None), h, weights)[0]


def reference(x, dy, w_gate, w_up, w_down):
    weights = dict(zip(NAMES, (w_gate, w_up, w_down), strict=True))

    def take(so_far, sequence):
        h, by_y = sequence
        _, back = jax.vjp(stack, weights, h)
        by_weights, by_h = back(by_y)
        return jax.tree.map(lambda total, term: total + term.astype(jnp.float32), so_far, by_weights), by_h

    none_yet = {name: jnp.zeros(w.shape, jnp.float32) for name, w in weights.items()}
    by_weights, by_x = lax.scan(take, none_yet, (x, dy))
    return (by_x, *(by_weights[name].astype(jnp.bfloat16) for name in NAMES))
```

```python
import functools
import math

import jax
import jax.numpy as jnp
from jax import lax
from jax.experimental import pallas as pl
from jax.experimental.pallas import tpu as pltpu
from jax.sharding import PartitionSpec as P

F32, BF16 = jnp.float32, jnp.bfloat16
MESH = pl.DeviceIdType.MESH
LANES, PIECE = 128, 32
PER = LANES // PIECE
NN, NT, TN = ((1,), (0,)), ((1,), (1,)), ((0,), (0,))
SIGNS = (1, -1)
VMEM_LIMIT = 62 * 1024 * 1024


def dot(a, b, dims=NN):
    return lax.dot_general(a, b, (dims, ((), ())), preferred_element_type=F32)


def scale_of(wide):
    return lax.rsqrt(jnp.mean(wide**2, -1, keepdims=True) + 1e-6)


def place(n):
    side = math.isqrt(n)
    me = lax.axis_index("dp")
    x, y = me // side, me % side

    def at(v, u, w):
        u, w = lax.rem(u + 2 * side, side), lax.rem(w + 2 * side, side)
        return u * side + w if v == 0 else w * side + u

    return me, side, ((x, y), (y, x)), at


def entry_barrier(n, partner=None):
    me, side, uw, at = place(n)
    barrier = pltpu.get_barrier_semaphore()
    (u, w), others = uw[0], 4
    for s in SIGNS:
        pl.semaphore_signal(barrier, inc=1, device_id={"dp": at(0, u + s, w)}, device_id_type=MESH)
        pl.semaphore_signal(barrier, inc=1, device_id={"dp": at(0, u, w + s)}, device_id_type=MESH)
    if partner is not None:
        pl.semaphore_signal(barrier, inc=1, device_id={"rep": partner}, device_id_type=MESH)
        others += 1
    return lambda: pl.semaphore_wait(barrier, others)


def regroup(pieces, lane):
    for k in range(PER):
        out = pieces[k]
        for q in range(PER):
            if q != k:
                out = jnp.where(lane == q, pltpu.roll(pieces[q], (PIECE * (q - k)) % LANES, 1), out)
        yield k, out


def gather_kernel(n, tile, x_ref, wg_ref, wu_ref, wd_ref, g_ref, h_ref, own, a_ref, acc, w_buf, send_sem, recv_sem, pair_send, pair_recv, own_sem, load_sem):
    layers, chunks = g_ref.shape[:2]
    height, width = own.shape[3:]
    depth = width
    tokens = x_ref.shape[0]
    me, side, uw, at = place(n)
    rep = lax.axis_index("rep")
    core = lax.rem(rep, 2)
    partner = rep + 1 - 2 * core
    half = chunks // 2
    units = layers * half
    entered = entry_barrier(n, partner)

    first = pl.multiple_of(core * height, height)
    lane = lax.broadcasted_iota(jnp.int32, (height, LANES), 1) // PIECE
    per_device = wg_ref.shape[2] // n
    tiles, groups = per_device // LANES, n // PER

    def fill(i, _):
        layer, rest = i // (tiles * groups), lax.rem(i, tiles * groups)
        t, u = rest // groups, lax.rem(rest, groups)
        for m, w in enumerate((wg_ref, wu_ref)):
            pieces = [
                w[layer, pl.ds(first, height), pl.ds(pl.multiple_of((PER * u + q) * per_device + t * LANES, LANES), LANES)].astype(F32)
                for q in range(PER)
            ]
            for k, out in regroup(pieces, lane):
                own[layer, PER * t + k, m, :, pl.ds(pl.multiple_of(u * LANES, LANES), LANES)] = out.astype(BF16)
        return 0

    def fill_down(i, _):
        layer, j = i // chunks, lax.rem(i, chunks)
        own[layer, j, 2] = wd_ref[layer, pl.ds(pl.multiple_of(j * 2 * height + first, height), height), :]
        return 0

    lax.fori_loop(0, layers * tiles * groups, fill, 0)
    lax.fori_loop(0, layers * chunks, fill_down, 0)
    keep = [pltpu.make_async_copy(own.at[layer], g_ref.at[layer, :, me, core], own_sem.at[layer]) for layer in range(layers)]
    for copy in keep:
        copy.start()
    entered()

    def norm(i, _):
        rows = pl.ds(pl.multiple_of(i * tile, tile), tile)
        wide = x_ref[rows].astype(F32)
        a_ref[rows] = (wide * scale_of(wide)).astype(BF16)
        acc[rows] = jnp.zeros((tile, depth), F32)
        return 0

    def place_of(k, v):
        return k // half, 2 * lax.rem(k, half) + v

    def block(k, v, d):
        layer, j = place_of(k, v)
        return g_ref.at[layer, j, d, core]

    def copy_to(k, v, d, device, src=None):
        return pltpu.make_async_remote_copy(
            src_ref=block(k, v, d) if src is None else src,
            dst_ref=block(k, v, d),
            send_sem=send_sem,
            recv_sem=recv_sem.at[k, v, d],
            device_id={"dp": device},
            device_id_type=MESH,
        )

    def await_block(k, v, d):
        copy_to(k, v, d, me).wait_recv()

    def begin(k):
        for v, (u, w) in enumerate(uw):
            layer, j = place_of(k, v)
            for s in SIGNS:
                copy_to(k, v, me, at(v, u + s, w), own.at[layer, j]).start()
                copy_to(k, v, me, at(v, u, w + s), own.at[layer, j]).start()

    def spread(k, v, d, u, w):
        for s in SIGNS:
            copy_to(k, v, d, at(v, u, w + s)).start()

    def pass_on(k, v, column, sign):
        u, w = uw[v]
        for s in SIGNS:
            await_block(k, v, at(v, u + column, w + s))
        copy_to(k, v, at(v, u + column, w - sign), at(v, u, w + sign)).start()

    def near(k):
        sign = 1 - 2 * lax.rem(k, 2)
        for v, (u, w) in enumerate(uw):
            for s in SIGNS:
                await_block(k, v, at(v, u + s, w))
            copy_to(k, v, at(v, u - sign, w), at(v, u + sign, w)).start()
            for s in SIGNS:
                spread(k, v, at(v, u + s, w), u, w)
            pass_on(k, v, 0, sign)

    def middle(k):
        sign = 1 - 2 * lax.rem(k, 2)
        for v, (u, w) in enumerate(uw):
            await_block(k, v, at(v, u + 2, w))
            spread(k, v, at(v, u + 2, w), u, w)
            pass_on(k, v, 1, -sign)
            pass_on(k, v, -1, sign)

    def far(k):
        sign = 1 - 2 * lax.rem(k, 2)
        for v, (u, w) in enumerate(uw):
            pass_on(k, v, 2, -sign)
            await_block(k, v, at(v, u, w + 2))

    def pair_copy(k):
        layer, j = place_of(k, 0)
        ref = g_ref.at[layer, pl.ds(j, 2), :, core]
        return pltpu.make_async_remote_copy(
            src_ref=ref, dst_ref=ref, send_sem=pair_send, recv_sem=pair_recv.at[k], device_id={"rep": partner}, device_id_type=MESH
        )

    def last(k):
        for v, (u, w) in enumerate(uw):
            for column in (1, -1, 2):
                await_block(k, v, at(v, u + column, w + 2))
        pair_copy(k).start()

    def load(k, v):
        layer, j = place_of(k, v)
        slot = 2 * lax.rem(k, 2) + v
        return pltpu.make_async_copy(g_ref.at[layer, j], w_buf.at[slot], load_sem.at[slot])

    def both(k):
        layer, j = place_of(k, 0)
        ref = g_ref.at[layer, pl.ds(j, 2), :, 1 - core]
        pltpu.make_async_remote_copy(
            src_ref=ref, dst_ref=ref, send_sem=pair_send, recv_sem=pair_recv.at[k], device_id={"rep": partner}, device_id_type=MESH
        ).wait_recv()

        @pl.when(k < half)
        def _():
            for v in range(2):
                load(k, v).start()

    def forward(k):
        for v in range(2):
            load(k, v).wait()
            slot = 2 * lax.rem(k, 2) + v

            def rows_of(i, _):
                rows = pl.ds(pl.multiple_of(i * tile, tile), tile)
                a = a_ref[rows]
                gate = dot(a, w_buf[slot, :, :, 0].reshape(depth, width))
                up = dot(a, w_buf[slot, :, :, 1].reshape(depth, width))
                hidden = (gate * jax.nn.sigmoid(gate) * up).astype(BF16)
                acc[rows] += dot(hidden, w_buf[slot, :, :, 2].reshape(width, depth))
                return 0

            lax.fori_loop(0, tokens // tile, rows_of, 0)

    def step(t, _):
        @pl.when(t < units)
        def _():
            begin(t)

        @pl.when(t == 0)
        def _():
            lax.fori_loop(0, tokens // tile, norm, 0)

        @pl.when(t == 2)
        def _():
            for copy in keep:
                copy.wait()

        for lag, stage in ((4, last), (3, far), (2, middle), (1, near), (5, both)):

            @pl.when((t >= lag) & (t < units + lag))
            def _(lag=lag, stage=stage):
                stage(t - lag)

        @pl.when((t >= 6) & (t < half + 6))
        def _():
            forward(t - 6)

        return 0

    lax.fori_loop(0, units + 6, step, 0)

    def result(i, _):
        rows = pl.ds(pl.multiple_of(i * tile, tile), tile)
        h_ref[rows] = x_ref[rows] + acc[rows].astype(BF16)
        return 0

    lax.fori_loop(0, tokens // tile, result, 0)
    for sem, blocks in ((send_sem, n - 1), (pair_send, n)):
        ref = g_ref.at[:, :, pl.ds(0, blocks), 0]
        pltpu.make_async_copy(ref, ref, sem).wait()


def gather(n, x, wg, wu, wd):
    (layers, height, _), depth = wg.shape, x.shape[1]
    width = n * PIECE
    chunks = wd.shape[1] // PIECE
    assert depth == width and height == PIECE and layers == 2
    tile = min(256, x.shape[0])
    vmem = pl.BlockSpec(memory_space=pltpu.VMEM)
    return pl.pallas_call(
        functools.partial(gather_kernel, n, tile),
        out_shape=(
            jax.ShapeDtypeStruct((layers, chunks, n, 2, 3, height // 2, width), BF16),
            jax.ShapeDtypeStruct(x.shape, BF16),
        ),
        in_specs=[vmem] * 4,
        out_specs=(pl.BlockSpec(memory_space=pl.ANY), vmem),
        scratch_shapes=[
            pltpu.VMEM((layers, chunks, 3, height // 2, width), BF16),
            pltpu.VMEM(x.shape, BF16),
            pltpu.VMEM(x.shape, F32),
            pltpu.VMEM((4, n, 2, 3, height // 2, width), BF16),
            pltpu.SemaphoreType.DMA,
            pltpu.SemaphoreType.DMA((layers * chunks // 2, 2, n)),
            pltpu.SemaphoreType.DMA,
            pltpu.SemaphoreType.DMA((layers * chunks // 2,)),
            pltpu.SemaphoreType.DMA((layers,)),
            pltpu.SemaphoreType.DMA((4,)),
        ],
        compiler_params=pltpu.CompilerParams(collective_id=0, has_side_effects=True, vmem_limit_bytes=VMEM_LIMIT),
        name="gather_forward",
    )(x, wg, wu, wd)


def backward_kernel(
    n, tile, x_ref, h_ref, dy_ref, g_ref, o_ref, dx_ref,
    a_ref, at_ref, d_ref, hid_ref, dg_ref, du_ref, dag, dau, w_buf, terms, sums, out_buf,
    raw1_s, raw1_r, run1_s, run1_r, raw2_s, raw2_r, run2_s, run2_r,
    load_sem, out_sem, raw1_ss, raw1_rs, run1_ss, run1_rs, raw2_ss, raw2_rs, run2_ss, run2_rs,
):
    layers, chunks = g_ref.shape[:2]
    tokens, depth = x_ref.shape
    width = w_buf.shape[-1]
    height = terms.shape[3]
    low, part = height // 2, width // 2
    me, side, uw, at = place(n)
    total = layers * chunks
    entered = entry_barrier(n)

    def load(t):
        slot = lax.rem(t, 2)
        return pltpu.make_async_copy(g_ref.at[layers - 1 - t // chunks, lax.rem(t, chunks)], w_buf.at[slot], load_sem.at[slot])

    load(0).start()

    def row_tiles(body):
        def once(i, _):
            body(pl.ds(pl.multiple_of(i * tile, tile), tile))
            return 0

        lax.fori_loop(0, tokens // tile, once, 0)

    def start_layer(source):
        def body(rows):
            wide = source[rows].astype(F32)
            a = wide * scale_of(wide)
            a_ref[rows] = a.astype(BF16)
            at_ref[:, rows] = a.T.astype(BF16)
            dag[rows] = jnp.zeros((tile, depth), F32)
            dau[rows] = jnp.zeros((tile, depth), F32)

        row_tiles(body)

    def end_layer(source, target):
        def body(rows):
            wide = source[rows].astype(F32)
            scale = scale_of(wide)
            da = (dag[rows].astype(BF16) + dau[rows].astype(BF16)).astype(F32)
            inner = jnp.sum(da * wide, -1, keepdims=True)
            by_h = da * scale - wide * (scale * scale * scale * inner / depth)
            target[rows] = d_ref[rows] + by_h.astype(BF16)

        row_tiles(body)

    def compute(t):
        slot, held = lax.rem(t, 2), lax.rem(t, 3)
        load(t).wait()

        @pl.when(t + 1 < total)
        def _():
            load(t + 1).start()

        def body(rows):
            a, d = a_ref[rows], d_ref[rows]
            wg = w_buf[slot, :, :, 0].reshape(depth, width)
            wu = w_buf[slot, :, :, 1].reshape(depth, width)
            wd = w_buf[slot, :, :, 2].reshape(width, depth)
            gate, up = dot(a, wg), dot(a, wu)
            by_hid = dot(d, wd, NT).astype(BF16).astype(F32)
            sig = jax.nn.sigmoid(gate)
            silu = gate * sig
            dg = (by_hid * up * (sig + silu * (1 - sig))).astype(BF16)
            du = (by_hid * silu).astype(BF16)
            hid_ref[rows] = (silu * up).astype(BF16)
            dg_ref[rows] = dg
            du_ref[rows] = du
            dag[rows] += dot(dg, wg, NT)
            dau[rows] += dot(du, wu, NT)

        row_tiles(body)
        step = n // 2
        for m, (left, right, dims) in enumerate(((at_ref, dg_ref, NN), (at_ref, du_ref, NN), (hid_ref, d_ref, TN))):
            for i in range(2):
                some = pl.ds(i * step * height, step * height)
                value = dot(left[some] if dims is NN else left[:, some], right[...], dims)
                terms[held, m, i * step : (i + 1) * step] = value.reshape(step, height, width)

    def rows_of(v):
        return slice(v * low, (v + 1) * low)

    def cols_of(h):
        return slice(h * part, (h + 1) * part)

    flows = [(v, i, s) for v in range(2) for i, s in enumerate(SIGNS)]

    def send(k, v, i, second, src, dst, src_sem, dst_sem):
        u, w = uw[v]
        s = SIGNS[i]
        device = at(v, u, w + s) if second else at(v, u + s, w)
        return pltpu.make_async_remote_copy(
            src_ref=src.at[lax.rem(k, 2), v, i],
            dst_ref=dst.at[lax.rem(k, 4), v, i],
            send_sem=src_sem.at[lax.rem(k, 2), v, i],
            recv_sem=dst_sem.at[lax.rem(k, 4), v, i],
            device_id={"dp": device},
            device_id_type=MESH,
        )

    raw1 = lambda k, v, i: send(k, v, i, False, raw1_s, raw1_r, raw1_ss, raw1_rs)
    run1 = lambda k, v, i: send(k, v, i, False, run1_s, run1_r, run1_ss, run1_rs)
    raw2 = lambda k, v, i: send(k, v, i, True, raw2_s, raw2_r, raw2_ss, raw2_rs)
    run2 = lambda k, v, i: send(k, v, i, True, run2_s, run2_r, run2_ss, run2_rs)

    def wait_all(kind, k):
        for v, i, _ in flows:
            kind(k, v, i).wait()

    def start_all(kind, k):
        for v, i, _ in flows:
            kind(k, v, i).start()

    def pack(t):
        held, slot = lax.rem(t, 3), lax.rem(t, 2)
        for v, i, s in flows:
            u = uw[v][0]
            for w in range(side):
                raw1_s[slot, v, i, 0, w] = terms[held, :, at(v, u + 2, w), rows_of(v), cols_of(i)].astype(BF16)
                raw1_s[slot, v, i, 1, w] = terms[held, :, at(v, u + s, w), rows_of(v), cols_of(1 - i)].astype(BF16)

    def add1(k):
        held, slot, got = lax.rem(k, 3), lax.rem(k, 2), lax.rem(k, 4)
        wait_all(raw1, k)
        for v, i, s in flows:
            u = uw[v][0]
            for w in range(side):
                own = terms[held, :, at(v, u + s, w), rows_of(v), cols_of(i)]
                run1_s[slot, v, i, w] = (own + raw1_r[got, v, i, 0, w].astype(F32)).astype(BF16)
        start_all(run1, k)

    def turn(k):
        held, slot, got = lax.rem(k, 3), lax.rem(k, 2), lax.rem(k, 4)
        wait_all(run1, k)
        for v, i, s in flows:
            u = uw[v][0]
            for w in range(side):
                own = terms[held, :, at(v, u, w), rows_of(v), cols_of(i)]
                sums[slot, v, i, w] = own + run1_r[got, v, i, w].astype(F32) + raw1_r[got, v, 1 - i, 1, w].astype(F32)
        for v, i, s in flows:
            w = uw[v][1]
            raw2_s[slot, v, i, 0] = sums[slot, v, i, lax.rem(w + 2, side)].astype(BF16)
            raw2_s[slot, v, i, 1] = sums[slot, v, 1 - i, lax.rem(w + s + side, side)].astype(BF16)
        start_all(raw2, k)

    def add2(k):
        slot, got = lax.rem(k, 2), lax.rem(k, 4)
        wait_all(raw2, k)
        for v, i, s in flows:
            w = uw[v][1]
            own = sums[slot, v, i, lax.rem(w + s + side, side)]
            run2_s[slot, v, i] = (own + raw2_r[got, v, i, 0].astype(F32)).astype(BF16)
        start_all(run2, k)

    def put(k):
        slot = lax.rem(k, 2)
        return pltpu.make_async_copy(out_buf.at[slot], o_ref.at[layers - 1 - k // chunks, lax.rem(k, chunks)], out_sem.at[slot])

    def finish(k):
        slot, got = lax.rem(k, 2), lax.rem(k, 4)
        wait_all(run2, k)

        @pl.when(k >= 2)
        def _():
            put(k - 2).wait()

        for v, i, s in flows:
            w = uw[v][1]
            value = sums[slot, v, i, w] + run2_r[got, v, i].astype(F32) + raw2_r[got, v, 1 - i, 1].astype(F32)
            out_buf[slot, :, rows_of(v), cols_of(i)] = value.astype(BF16)
        put(k).start()

    def copy_d(rows):
        d_ref[rows] = dy_ref[rows]

    row_tiles(copy_d)
    start_layer(h_ref)
    entered()

    def step(t, _):
        for lag, stage in ((5, finish), (4, add2), (3, turn), (2, add1)):

            @pl.when((t >= lag) & (t < total + lag))
            def _(lag=lag, stage=stage):
                stage(t - lag)

        @pl.when(t == chunks)
        def _():
            end_layer(h_ref, d_ref)
            start_layer(x_ref)

        @pl.when(t < total)
        def _():
            compute(t)
            pack(t)
            start_all(raw1, t)

        @pl.when(t == total)
        def _():
            end_layer(x_ref, dx_ref)

        return 0

    lax.fori_loop(0, total + 6, step, 0)
    for k in (total - 2, total - 1):
        put(k).wait()


def backward(n, x, h, dy, g):
    layers, chunks, _, _, _, low, width = g.shape
    tokens, depth = x.shape
    side, part = math.isqrt(n), width // 2
    tile = min(256, tokens)
    vmem = pl.BlockSpec(memory_space=pltpu.VMEM)
    anywhere = pl.BlockSpec(memory_space=pl.ANY)
    pair = lambda count, *rest, dtype=BF16: pltpu.VMEM((count, 2, 2, *rest), dtype)
    sems = lambda count: pltpu.SemaphoreType.DMA((count, 2, 2))
    block = (3, low, part)
    return pl.pallas_call(
        functools.partial(backward_kernel, n, tile),
        out_shape=(
            jax.ShapeDtypeStruct((layers, chunks, 3, 2 * low, width), BF16),
            jax.ShapeDtypeStruct(x.shape, BF16),
        ),
        in_specs=[vmem, vmem, vmem, anywhere],
        out_specs=(anywhere, vmem),
        scratch_shapes=[
            pltpu.VMEM(x.shape, BF16),
            pltpu.VMEM(x.shape[::-1], BF16),
            pltpu.VMEM(x.shape, BF16),
            *[pltpu.VMEM((tokens, width), BF16)] * 3,
            *[pltpu.VMEM(x.shape, F32)] * 2,
            pltpu.VMEM((2, *g.shape[2:]), BF16),
            pltpu.VMEM((3, 3, n, 2 * low, width), F32),
            pair(2, side, *block, dtype=F32),
            pltpu.VMEM((2, 3, 2 * low, width), BF16),
            pair(2, 2, side, *block), pair(4, 2, side, *block),
            pair(2, side, *block), pair(4, side, *block),
            pair(2, 2, *block), pair(4, 2, *block),
            pair(2, *block), pair(4, *block),
            pltpu.SemaphoreType.DMA((2,)),
            pltpu.SemaphoreType.DMA((2,)),
            *[sems(2), sems(4)] * 4,
        ],
        compiler_params=pltpu.CompilerParams(collective_id=1, has_side_effects=True, vmem_limit_bytes=VMEM_LIMIT),
        name="backward_reduce",
    )(x, h, dy, g)


def restore_kernel(n, o_ref, dg_ref, du_ref):
    layers, chunks, _, height, width = o_ref.shape
    per_device = dg_ref.shape[2] // n
    tiles, groups = per_device // LANES, n // PER
    lane = lax.broadcasted_iota(jnp.int32, (height, LANES), 1) // PIECE

    def body(i, _):
        layer, rest = i // (tiles * groups), lax.rem(i, tiles * groups)
        t, u = rest // groups, lax.rem(rest, groups)
        for m, w in enumerate((dg_ref, du_ref)):
            pieces = [o_ref[layer, PER * t + k, m, :, pl.ds(pl.multiple_of(u * LANES, LANES), LANES)].astype(F32) for k in range(PER)]
            for q, out in regroup(pieces, lane):
                w[layer, :, pl.ds(pl.multiple_of((PER * u + q) * per_device + t * LANES, LANES), LANES)] = out.astype(BF16)
        return 0

    lax.fori_loop(0, layers * tiles * groups, body, 0)


def restore(n, o):
    layers, chunks, _, height, width = o.shape
    shape = jax.ShapeDtypeStruct((layers, height, chunks * width), BF16)
    vmem = pl.BlockSpec(memory_space=pltpu.VMEM)
    return pl.pallas_call(
        functools.partial(restore_kernel, n),
        out_shape=(shape, shape),
        in_specs=[vmem],
        out_specs=(vmem, vmem),
        compiler_params=pltpu.CompilerParams(vmem_limit_bytes=32 * 1024 * 1024),
        name="restore_order",
    )(o)


def solution(mesh):
    n = mesh.shape["dp"]

    def step(x, dy, wg, wu, wd):
        x, dy = x[0], dy[0]
        g, h = gather(n, x, wg, wu, wd)
        o, dx = backward(n, x, h, dy, g)
        dg, du = restore(n, o)
        return dx[None], dg, du, o[:, :, 2].reshape(wd.shape)

    tokens, rows, out = P(("rep", "dp"), None, None), P(None, "dp", None), P("rep", "dp", None)
    return jax.shard_map(step, mesh=mesh, in_specs=(tokens, tokens, rows, rows, rows), out_specs=(tokens, out, out, out), check_vma=False)
```

```python
import functools
import math

import jax
import jax.numpy as jnp
from jax import lax
from jax.experimental import pallas as pl
from jax.experimental.pallas import tpu as pltpu
from jax.sharding import PartitionSpec as P

F32, BF16 = jnp.float32, jnp.bfloat16
MESH = pl.DeviceIdType.MESH
LANES, PIECE = 128, 32
PER = LANES // PIECE
NN, NT, TN = ((1,), (0,)), ((1,), (1,)), ((0,), (0,))
SIGNS = (1, -1)
VMEM_LIMIT = 67_043_328


def dot(a, b, dims=NN):
    return lax.dot_general(a, b, (dims, ((), ())), preferred_element_type=F32)


def scale_of(wide):
    return lax.rsqrt(jnp.mean(wide**2, -1, keepdims=True) + 1e-6)


LEAD, GAP, AHEAD, DY = 0, 0, 4, 4


def place(n):
    side = math.isqrt(n)
    me = lax.axis_index("dp")
    x, y = me // side, lax.rem(me, side)

    def at(v, u, w):
        u, w = lax.rem(u + 2 * side, side), lax.rem(w + 2 * side, side)
        return u * side + w if v == 0 else w * side + u

    return me, side, ((x, y), (y, x)), at


def regroup(pieces, lane):
    for k in range(PER):
        out = pieces[k]
        for q in range(PER):
            if q != k:
                out = jnp.where(lane == q, pltpu.roll(pieces[q], (PIECE * (q - k)) % LANES, 1), out)
        yield k, out


def kernel(
    n, x_in, dy_in, wg_in, wu_in, wd_in, dx_out, dwg_out, dwu_out, dwd_out, g_ref,
    local, own, x_ref, h_ref, a_ref, at_ref, d_ref, shared, hid_ref, dg_ref, du_ref, dag, dau, w_buf, terms, mixed, result, result_down,
    sum_p, sum_q, swap_s, swap_r, raw_p_s, raw_p_r, run_p_s, run_p_r, raw_q_s, raw_q_r, run_q_s, run_q_r, turn_s, turn_r, last_s, last_r,
    in_sem, local_sem, down_sem, keep_sem, send_sem, recv_sem, pair_send, pair_recv, load_sem, out_sem, share_ss, share_rs,
    swap_ss, swap_rs, raw_p_ss, raw_p_rs, run_p_ss, run_p_rs, raw_q_ss, raw_q_rs, run_q_ss, run_q_rs, turn_ss, turn_rs, last_ss, last_rs,
):
    layers, chunks = g_ref.shape[:2]
    low, width = own.shape[3:]
    height, part = 2 * low, width // 2
    tokens, depth = x_ref.shape
    me, side, uw, at = place(n)
    x, y = uw[0]
    mate = x + 1 - 2 * lax.rem(x, 2)
    twin = lax.rem(x + 2 * lax.rem(x, 2) - 1 + side, side)
    twin_mate = twin + 1 - 2 * lax.rem(twin, 2)
    parity = lax.rem((x + 1) // 2, 2)
    rep = lax.axis_index("rep")
    core = lax.rem(rep, 2)
    partner = rep + 1 - 2 * core
    half = chunks // 2
    units = layers * half
    opening = half + 6 + GAP
    ahead, by_y = AHEAD * half // 8, DY * half // 8
    turnover = LEAD + half

    barrier = pltpu.get_barrier_semaphore()
    for s in SIGNS:
        pl.semaphore_signal(barrier, inc=1, device_id={"dp": at(0, x + s, y)}, device_id_type=MESH)
        pl.semaphore_signal(barrier, inc=1, device_id={"dp": at(0, x, y + s)}, device_id_type=MESH)
    pl.semaphore_signal(barrier, inc=1, device_id={"rep": partner}, device_id_type=MESH)


    first = pl.multiple_of(core * low, low)

    def fetch(layer, m):
        return pltpu.make_async_copy((wg_in, wu_in)[m].at[layer, pl.ds(first, low)], local.at[layer, m], local_sem.at[layer, m])

    def fetch_down(layer):
        return pltpu.make_async_copy(wd_in.at[layer, :, pl.ds(first, low)], own.at[layer, :, 2], down_sem.at[layer])

    inputs = [pltpu.make_async_copy(x_in, x_ref, in_sem.at[0]), pltpu.make_async_copy(dy_in, d_ref.at[pl.ds(0, tokens)], in_sem.at[1])]
    for layer in range(layers):
        for m in range(2):
            fetch(layer, m).start()
        fetch_down(layer).start()
    for copy in inputs:
        copy.start()

    lane_low = lax.broadcasted_iota(jnp.int32, (low, LANES), 1) // PIECE
    lane_high = lax.broadcasted_iota(jnp.int32, (height, LANES), 1) // PIECE
    per_device = wg_in.shape[2] // n
    tiles, groups = per_device // LANES, n // PER

    def columns(u, q, t):
        return pl.ds(pl.multiple_of((PER * u + q) * per_device + t * LANES, LANES), LANES)

    def tile_of(u):
        return pl.ds(pl.multiple_of(u * LANES, LANES), LANES)

    def keep(i):
        layer, some = i // tiles, pl.ds(PER * lax.rem(i, tiles), PER)
        return pltpu.make_async_copy(own.at[layer, some], g_ref.at[layer, some, me, core], keep_sem.at[i])

    def fill(i):
        layer, t = i // tiles, lax.rem(i, tiles)

        @pl.when(t == 0)
        def _():
            for m in range(2):
                fetch(layer, m).wait()
            fetch_down(layer).wait()

        def once(u, _):
            for m in range(2):
                pieces = [local[layer, m, :, columns(u, q, t)].astype(F32) for q in range(PER)]
                for k, out in regroup(pieces, lane_low):
                    own[layer, PER * t + k, m, :, tile_of(u)] = out.astype(BF16)
            return 0

        lax.fori_loop(0, groups, once, 0)
        keep(i).start()


    def place_of(k, v):
        return k // half, 2 * lax.rem(k, half) + v

    def block(k, v, d):
        layer, j = place_of(k, v)
        return g_ref.at[layer, j, d, core]

    def copy_to(k, v, d, device, src=None):
        return pltpu.make_async_remote_copy(
            src_ref=block(k, v, d) if src is None else src,
            dst_ref=block(k, v, d),
            send_sem=send_sem,
            recv_sem=recv_sem.at[k, v, d],
            device_id={"dp": device},
            device_id_type=MESH,
        )

    def await_block(k, v, d):
        copy_to(k, v, d, me).wait_recv()

    def begin(k):
        for v, (u, w) in enumerate(uw):
            layer, j = place_of(k, v)
            for s in SIGNS:
                copy_to(k, v, me, at(v, u + s, w), own.at[layer, j]).start()
                copy_to(k, v, me, at(v, u, w + s), own.at[layer, j]).start()

    def spread(k, v, d, u, w):
        for s in SIGNS:
            copy_to(k, v, d, at(v, u, w + s)).start()

    def pass_on(k, v, column, sign):
        u, w = uw[v]
        for s in SIGNS:
            await_block(k, v, at(v, u + column, w + s))
        copy_to(k, v, at(v, u + column, w - sign), at(v, u, w + sign)).start()

    def ways(k):
        sign, later = 1 - 2 * lax.rem(k, 2), k // half
        across = (2 * lax.rem(x, 2) - 1) * (1 - 2 * later)
        return across, sign, across, -sign

    def near(k):
        signs = ways(k)
        for v, (u, w) in enumerate(uw):
            for s in SIGNS:
                await_block(k, v, at(v, u + s, w))
            copy_to(k, v, at(v, u - signs[v], w), at(v, u + signs[v], w)).start()
            for s in SIGNS:
                spread(k, v, at(v, u + s, w), u, w)
            pass_on(k, v, 0, signs[1 - v])

    def middle(k):
        signs = ways(k)
        for v, (u, w) in enumerate(uw):
            await_block(k, v, at(v, u + 2, w))
            spread(k, v, at(v, u + 2, w), u, w)
            pass_on(k, v, 1, signs[3 - v])
            pass_on(k, v, -1, signs[1 - v])

    def far(k):
        signs = ways(k)
        for v, (u, w) in enumerate(uw):
            pass_on(k, v, 2, signs[3 - v])
            await_block(k, v, at(v, u, w + 2))

    def pair_copy(k, whose):
        layer, j = place_of(k, 0)
        ref = g_ref.at[layer, pl.ds(j, 2), :, whose]
        return pltpu.make_async_remote_copy(
            src_ref=ref, dst_ref=ref, send_sem=pair_send, recv_sem=pair_recv.at[k], device_id={"rep": partner}, device_id_type=MESH
        )

    def last(k):
        for v, (u, w) in enumerate(uw):
            for column in (1, -1, 2):
                await_block(k, v, at(v, u + column, w + 2))

        @pl.when(lax.rem(k, PER // 2) == 0)
        def _():
            keep(k // (PER // 2)).wait()

        pair_copy(k, core).start()


    def load(layer, j, slot):
        return pltpu.make_async_copy(g_ref.at[layer, j], w_buf.at[slot], load_sem.at[slot])

    def load_unit(k, v):
        return load(0, 2 * k + v, 2 * lax.rem(k, 2) + v)

    def load_other(o):
        return load(layers - 1 - o // half, 2 * lax.rem(o, half) + 1 - parity, lax.rem(o, 2))

    def load_mine(c):
        return load(layers - 1 - c // half, 2 * lax.rem(c, half) + parity, 2 + lax.rem(c, 2))

    def both(k):
        pair_copy(k, 1 - core).wait_recv()

        @pl.when(k < half)
        def _():
            for v in range(2):
                load_unit(k, v).start()

    mine_rows, mate_rows = pl.ds(0, tokens), pl.ds(tokens, tokens)

    def matrices(slot):
        return [w_buf[slot, :, :, m].reshape(depth, width) for m in range(3)]

    def sigmoid(z):
        return 0.5 * jnp.tanh(0.5 * z) + 0.5

    def forward(k):
        for rows, total in ((mine_rows, dag), (mate_rows, dau)):
            if rows is mate_rows:

                @pl.when(k == 0)
                def _():
                    share_all(0).wait_recv()
                    wide = shared[0].astype(F32)
                    a_ref[mate_rows] = (wide * scale_of(wide)).astype(BF16)

            for v in range(2):
                if rows is mine_rows:
                    load_unit(k, v).wait()
                wg, wu, wd = matrices(2 * lax.rem(k, 2) + v)
                a = a_ref[rows]
                gate, up = dot(a, wg), dot(a, wu)
                total[...] += dot((gate * sigmoid(gate) * up).astype(BF16), wd)


    def share(kind, piece, count=1):
        rows = pl.ds(piece * (tokens // half), count * (tokens // half))
        source = (x_ref, h_ref, d_ref, d_ref)[kind]
        return pltpu.make_async_remote_copy(
            src_ref=source.at[rows],
            dst_ref=shared.at[kind, rows],
            send_sem=share_ss.at[kind],
            recv_sem=share_rs.at[kind],
            device_id={"dp": at(0, mate, y)},
            device_id_type=MESH,
        )

    def share_all(kind):
        return share(kind, 0, half)


    def normed(source, rows):
        wide = source.astype(F32)
        a = wide * scale_of(wide)
        a_ref[rows] = a.astype(BF16)
        at_ref[:, rows] = a.T.astype(BF16)

    def start_layer(source):
        normed(source[...], mine_rows)
        dag[...] = jnp.zeros_like(dag)
        dau[...] = jnp.zeros_like(dau)

    def meet(kind, by_kind):
        normed(shared[kind], mate_rows)
        share_all(by_kind).wait_recv()
        d_ref[mate_rows] = shared[by_kind]

    def end_layer(source):
        wide = source[...].astype(F32)
        scale = scale_of(wide)
        da = (dag[...].astype(BF16) + dau[...].astype(BF16)).astype(F32)
        inner = jnp.sum(da * wide, -1, keepdims=True)
        by_h = da * scale - wide * (scale * scale * scale * inner / depth)
        d_ref[mine_rows] = d_ref[mine_rows] + by_h.astype(BF16)

    def by_hidden(slot, rows, kept):
        wg, wu, wd = matrices(slot)
        a, d = a_ref[rows], d_ref[rows]
        gate, up = dot(a, wg), dot(a, wu)
        by_hid = dot(d, wd, NT).astype(BF16).astype(F32)
        sig = sigmoid(gate)
        silu = gate * sig
        dg = (by_hid * up * (sig + silu * (1 - sig))).astype(BF16)
        du = (by_hid * silu).astype(BF16)
        if kept:
            hid_ref[rows] = (silu * up).astype(BF16)
            dg_ref[rows] = dg
            du_ref[rows] = du
        return dg, du, wg, wu

    def own_part(slot, kept):
        dg, du, wg, wu = by_hidden(slot, mine_rows, kept)
        dag[...] += dot(dg, wg, NT)
        dau[...] += dot(du, wu, NT)

    def compute(c):
        held, slot = lax.rem(c, 3), 2 + lax.rem(c, 2)
        load_mine(c).wait()
        own_part(slot, True)
        by_hidden(slot, mate_rows, True)
        step = n // 2
        for m, (left, right, dims) in enumerate(((at_ref, dg_ref, NN), (at_ref, du_ref, NN), (hid_ref, d_ref, TN))):
            for i in range(2):
                some = pl.ds(i * step * height, step * height)
                value = dot(left[some] if dims is NN else left[:, some], right[...], dims)
                terms[held, m, i * step : (i + 1) * step] = value.reshape(step, height, width)


    P_ROWS, Q_ROWS = slice(0, low), slice(low, height)
    MINE, THEIRS = (x, mate), (twin, twin_mate)

    def cols_of(h):
        return slice(h * part, (h + 1) * part)

    def remote(k, src, dst, src_sem, dst_sem, device, *index):
        return pltpu.make_async_remote_copy(
            src_ref=src.at[(lax.rem(k, 2), *index)],
            dst_ref=dst.at[(lax.rem(k, 4), *index)],
            send_sem=src_sem.at[(lax.rem(k, 2), *index)],
            recv_sem=dst_sem.at[(lax.rem(k, 4), *index)],
            device_id={"dp": device},
            device_id_type=MESH,
        )

    def down_the_column(src, dst, src_sem, dst_sem):
        return lambda k: [remote(k, src, dst, src_sem, dst_sem, at(0, x, y + s), i) for i, s in enumerate(SIGNS)]

    swap = lambda k: [remote(k, swap_s, swap_r, swap_ss, swap_rs, at(0, twin, y))]
    turn = lambda k: [remote(k, turn_s, turn_r, turn_ss, turn_rs, at(0, twin, y))]
    hand = lambda k: [remote(k, last_s, last_r, last_ss, last_rs, at(0, mate, y))]
    raw_p = down_the_column(raw_p_s, raw_p_r, raw_p_ss, raw_p_rs)
    run_p = down_the_column(run_p_s, run_p_r, run_p_ss, run_p_rs)
    raw_q = down_the_column(raw_q_s, raw_q_r, raw_q_ss, raw_q_rs)
    run_q = down_the_column(run_q_s, run_q_r, run_q_ss, run_q_rs)

    def go(copies):
        for copy in copies:
            copy.start()

    def arrive(copies):
        for copy in copies:
            copy.wait()

    def row(w):
        return lax.rem(w + 2 * side, side)

    def slots(k):
        return lax.rem(k, 3), lax.rem(k, 2), lax.rem(k, 4)

    def pack(c):
        held, slot, _ = slots(c)
        for e, column in enumerate(THEIRS):
            for w in range(side):
                swap_s[slot, e, w] = terms[held, :, at(0, column, w), P_ROWS].astype(BF16)
        go(swap(c))
        for i, s in enumerate(SIGNS):
            for u in range(side):
                raw_q_s[slot, i, 0, u] = terms[held, :, at(0, u, y + 2), Q_ROWS, cols_of(i)].astype(BF16)
                raw_q_s[slot, i, 1, u] = terms[held, :, at(0, u, y + s), Q_ROWS, cols_of(1 - i)].astype(BF16)
        go(raw_q(c))

    def stage1(c):
        held, slot, got = slots(c)
        arrive(swap(c))
        for e, column in enumerate(MINE):
            for w in range(side):
                sum_p[slot, e, w] = terms[held, :, at(0, column, w), P_ROWS] + swap_r[got, e, w].astype(F32)
        for i, s in enumerate(SIGNS):
            for e in range(2):
                raw_p_s[slot, i, 0, e] = sum_p[slot, e, row(y + 2), :, :, cols_of(i)].astype(BF16)
                raw_p_s[slot, i, 1, e] = sum_p[slot, e, row(y + s), :, :, cols_of(1 - i)].astype(BF16)
        go(raw_p(c))
        arrive(raw_q(c))
        for i, s in enumerate(SIGNS):
            for u in range(side):
                value = terms[held, :, at(0, u, y + s), Q_ROWS, cols_of(i)] + raw_q_r[got, i, 0, u].astype(F32)
                run_q_s[slot, i, u] = value.astype(BF16)
        go(run_q(c))

    def stage2(c):
        held, slot, got = slots(c)
        arrive(raw_p(c))
        for i, s in enumerate(SIGNS):
            for e in range(2):
                value = sum_p[slot, e, row(y + s), :, :, cols_of(i)] + raw_p_r[got, i, 0, e].astype(F32)
                run_p_s[slot, i, e] = value.astype(BF16)
        go(run_p(c))
        arrive(run_q(c))
        for i in range(2):
            for e in range(2):
                for column, mine in ((MINE[e], True), (THEIRS[e], False)):
                    value = terms[held, :, at(0, column, y), Q_ROWS, cols_of(i)]
                    value = value + run_q_r[got, i, column].astype(F32) + raw_q_r[got, 1 - i, 1, column].astype(F32)
                    if mine:
                        sum_q[slot, e, :, :, cols_of(i)] = value
                    else:
                        turn_s[slot, e, :, :, cols_of(i)] = value.astype(BF16)
        go(turn(c))

    def own_chunk(c, other):
        return layers - 1 - c // half, 2 * lax.rem(c, half) + (1 - parity if other else parity)

    def settle(c, value, rows, cols):
        layer, j = own_chunk(c, False)
        mixed[:, lax.rem(j, PER), rows, cols] = value[:2]
        result_down[layer, j, rows, cols] = value[2]

    def stage3(c):
        held, slot, got = slots(c)
        arrive(run_p(c))
        for i in range(2):
            for e in range(2):
                value = sum_p[slot, e, y, :, :, cols_of(i)] + run_p_r[got, i, e].astype(F32) + raw_p_r[got, 1 - i, 1, e].astype(F32)
                if e == 0:
                    settle(c, value.astype(BF16), P_ROWS, cols_of(i))
                else:
                    last_s[slot, :, P_ROWS, cols_of(i)] = value.astype(BF16)
        arrive(turn(c))
        for e in range(2):
            value = (sum_q[slot, e] + turn_r[got, e].astype(F32)).astype(BF16)
            if e == 0:
                settle(c, value, Q_ROWS, slice(0, width))
            else:
                last_s[slot, :, Q_ROWS] = value
        go(hand(c))

    def put(layer):
        return [
            pltpu.make_async_copy(src.at[layer], dst.at[layer], out_sem.at[layer, m])
            for m, (src, dst) in enumerate(((result.at[0], dwg_out), (result.at[1], dwu_out), (result_down, dwd_out)))
        ]

    def stage4(c):
        _, _, got = slots(c)
        layer, j = own_chunk(c, True)
        arrive(hand(c))
        mixed[:, lax.rem(j, PER)] = last_r[got, :2]
        result_down[layer, j] = last_r[got, 2]

        @pl.when(lax.rem(c, PER // 2) == PER // 2 - 1)
        def _():
            def once(u, _):
                for m in range(2):
                    pieces = [mixed[m, q, :, tile_of(u)].astype(F32) for q in range(PER)]
                    for q, out in regroup(pieces, lane_high):
                        result[m, layer, :, columns(u, q, j // PER)] = out.astype(BF16)
                return 0

            lax.fori_loop(0, groups, once, 0)

        @pl.when(lax.rem(c, half) == half - 1)
        def _():
            for copy in put(layer):
                copy.start()

    def unit_at(t):
        q = t // (half + GAP)
        return t - GAP * q, (t >= 0) & (t < 2 * half + GAP) & (t - q * (half + GAP) < half)

    def mine_at(r):
        r = r - LEAD
        q = (r + 1024 - half - ahead) // 1024
        c = r - q * ahead
        return c, (r >= 0) & (r - q * (half + ahead) < half), (r >= 0) & ((r < half) | (q == 1))

    def other_at(r):
        late = r - turnover
        q = late // (half + ahead)
        return (r, (r >= 0) & (r < half)), (half + late - q * half, ((late >= 0) & (late < ahead)) | ((late >= half + ahead) & (late < 2 * half)))

    fill(0)
    pl.semaphore_wait(barrier, 5)

    def stages_at(t, *stages):
        for lag, stage in stages:
            k, here = unit_at(t - lag)

            @pl.when((t >= lag) & here)
            def _(k=k, stage=stage):
                stage(k)

    def step(t, _):
        r = t - opening
        (o, early), (o_late, late) = other_at(r)
        (o_soon, soon), (o_next, next_late) = other_at(r + 1)
        c, mine, going = mine_at(r)
        c_next, mine_next, _ = mine_at(r + 1)

        @pl.when(r == turnover)
        def _():
            share_all(2).wait_send()
            end_layer(h_ref)
            start_layer(x_ref)
            share_all(3).start()

        @pl.when(mine_next & (c_next >= half))
        def _():
            load_mine(c_next).start()

        for lag, stage in ((5, stage4), (4, stage3), (3, stage2), (2, stage1)):

            @pl.when(going & (c >= lag) & (c - lag < 2 * half))
            def _(lag=lag, stage=stage):
                stage(c - lag)

        @pl.when(next_late)
        def _():
            load_other(o_next).start()

        @pl.when(early | late)
        def _():
            chunk = o - (o - o_late) * ((r + 2 * half) // (turnover + 2 * half))
            load_other(chunk).wait()
            own_part(lax.rem(chunk, 2), False)

        stages_at(t, (5, both), (0, begin), (1, near), (2, middle), (3, far), (4, last))

        @pl.when(mine_next & (c_next < half))
        def _():
            load_mine(c_next).start()

        @pl.when(soon)
        def _():
            load_other(o_soon).start()

        coming, here = unit_at(t + 1)

        @pl.when(here & (lax.rem(coming, PER // 2) == 0))
        def _():
            fill(coming // (PER // 2))

        @pl.when(t == 0)
        def _():
            for copy in inputs:
                copy.wait()
            wide = x_ref[...].astype(F32)
            a_ref[mine_rows] = (wide * scale_of(wide)).astype(BF16)
            dag[...] = jnp.zeros_like(dag)
            dau[...] = jnp.zeros_like(dau)

        @pl.when(t < half // 2)
        def _():
            share(0, 2 * t, 2).start()

        @pl.when((t >= by_y) & (t < by_y + half))
        def _():
            share(2, t - by_y).start()

        @pl.when((t >= 5) & (t < half + 5))
        def _():
            forward(t - 5)

        @pl.when(t == half + 4)
        def _():
            h_ref[...] = x_ref[...] + dag[...].astype(BF16)
            shared[1] = shared[0] + dau[...].astype(BF16)
            start_layer(h_ref)

        @pl.when(r == LEAD)
        def _():
            meet(1, 2)

        @pl.when(r == turnover + ahead)
        def _():
            meet(0, 3)

        @pl.when((r >= LEAD) & mine)
        def _():
            compute(c)
            pack(c)

        @pl.when(r == turnover + 2 * half)
        def _():
            share_all(3).wait_send()
            end_layer(x_ref)
            pltpu.make_async_copy(d_ref.at[mine_rows], dx_out, in_sem.at[0]).start()

        return 0

    lax.fori_loop(0, opening + turnover + max(2 * half + 1, ahead + half + 5), step, 0)
    share_all(0).wait_send()
    pltpu.make_async_copy(d_ref.at[mine_rows], dx_out, in_sem.at[0]).wait()
    for layer in range(layers):
        for copy in put(layer):
            copy.wait()
    for sem, blocks in ((send_sem, n - 1), (pair_send, n)):
        ref = g_ref.at[:, :, pl.ds(0, blocks), 0]
        pltpu.make_async_copy(ref, ref, sem).wait()


def copy_kernel(*refs):
    count = (len(refs) - 2) // 3
    given, got, held, (in_sem, out_sem) = refs[:count], refs[count : 2 * count], refs[2 * count : 3 * count], refs[3 * count :]
    come = [pltpu.make_async_copy(a, b, in_sem.at[i]) for i, (a, b) in enumerate(zip(given, held, strict=True))]
    leave = [pltpu.make_async_copy(a, b, out_sem.at[i]) for i, (a, b) in enumerate(zip(held, got, strict=True))]
    for copy in come:
        copy.start()
    for first, second in zip(come, leave, strict=True):
        first.wait()
        second.start()
    for copy in leave:
        copy.wait()


def copied(*arrays):
    anywhere = pl.BlockSpec(memory_space=pl.ANY)
    return pl.pallas_call(
        copy_kernel,
        out_shape=[jax.ShapeDtypeStruct(a.shape, a.dtype) for a in arrays],
        in_specs=[anywhere] * len(arrays),
        out_specs=[anywhere] * len(arrays),
        scratch_shapes=[*[pltpu.VMEM(a.shape, a.dtype) for a in arrays], *[pltpu.SemaphoreType.DMA((len(arrays),))] * 2],
        compiler_params=pltpu.CompilerParams(vmem_limit_bytes=VMEM_LIMIT),
        name="copied",
    )(*arrays)


def run(n, x, dy, wg, wu, wd):
    (layers, height, local_width), (tokens, depth) = wg.shape, x.shape
    width = n * PIECE
    chunks = wd.shape[1] // PIECE
    assert depth == width and height == PIECE and layers == 2
    low, side, part = height // 2, math.isqrt(n), width // 2
    anywhere = pl.BlockSpec(memory_space=pl.ANY)
    sems = lambda *counts: pltpu.SemaphoreType.DMA(counts)
    bf16, f32 = (lambda *dims: pltpu.VMEM(dims, BF16)), (lambda *dims: pltpu.VMEM(dims, F32))
    whole, block = (3, low, width), (3, low, part)
    piece = (n, 2, 3, low, width)
    shape = lambda *dims: jax.ShapeDtypeStruct(dims, BF16)
    down = (layers, chunks, PIECE, depth)
    slots = lambda *dims: [bf16(2, *dims), bf16(4, *dims)]
    *results, _ = pl.pallas_call(
        functools.partial(kernel, n),
        out_shape=(shape(*x.shape), shape(*wg.shape), shape(*wu.shape), shape(*down), shape(layers, chunks, *piece)),
        in_specs=[anywhere] * 5,
        out_specs=(anywhere,) * 5,
        scratch_shapes=[
            bf16(layers, 2, low, local_width),
            bf16(layers, chunks, *whole),
            *[bf16(*x.shape)] * 2,
            bf16(2 * tokens, depth), bf16(depth, 2 * tokens), bf16(2 * tokens, depth),
            bf16(4, tokens, depth),
            *[bf16(2 * tokens, width)] * 3,
            *[f32(*x.shape)] * 2,
            bf16(4, *piece),
            f32(3, 3, n, height, width),
            bf16(2, PER, height, width), bf16(2, *wg.shape), bf16(*down),
            f32(2, 2, side, *whole), f32(2, 2, *whole),
            *slots(2, side, *whole),
            *slots(2, 2, 2, *block), *slots(2, 2, *block),
            *slots(2, 2, side, *block), *slots(2, side, *block),
            *slots(2, *whole), *slots(3, height, width),
            sems(2), sems(layers, 2), sems(layers), sems(layers * chunks // PER),
            pltpu.SemaphoreType.DMA, sems(layers * chunks // 2, 2, n), pltpu.SemaphoreType.DMA, sems(layers * chunks // 2),
            sems(4), sems(layers, 3), sems(4), sems(4),
            sems(2), sems(4), *[sems(2, 2), sems(4, 2)] * 4, *[sems(2), sems(4)] * 2,
        ],
        compiler_params=pltpu.CompilerParams(collective_id=0, has_side_effects=True, vmem_limit_bytes=VMEM_LIMIT),
        name="layers",
    )(x, dy, wg, wu, wd.reshape(down))
    dx, dwg, dwu, dwd = copied(*results)
    return dx, dwg, dwu, dwd.reshape(wd.shape)


def solution(mesh):
    n = mesh.shape["dp"]

    def step(x, dy, wg, wu, wd):
        dx, *by_weights = run(n, x[0], dy[0], wg, wu, wd)
        return (dx[None], *by_weights)

    tokens, rows, out = P(("rep", "dp"), None, None), P(None, "dp", None), P("rep", "dp", None)
    return jax.shard_map(step, mesh=mesh, in_specs=(tokens, tokens, rows, rows, rows), out_specs=(tokens, out, out, out), check_vma=False)
```

```python
import functools
import math

import jax
import jax.numpy as jnp
from jax import lax
from jax.experimental import pallas as pl
from jax.experimental.pallas import tpu as pltpu
from jax.sharding import PartitionSpec as P

F32, BF16 = jnp.float32, jnp.bfloat16
MESH = pl.DeviceIdType.MESH
LANES, PIECE = 128, 32
PER = LANES // PIECE
NN, NT, TN = ((1,), (0,)), ((1,), (1,)), ((0,), (0,))
SIGNS = (1, -1)
VMEM_LIMIT = 67_043_328


def dot(a, b, dims=NN):
    return lax.dot_general(a, b, (dims, ((), ())), preferred_element_type=F32)


def scale_of(wide):
    return lax.rsqrt(jnp.mean(wide**2, -1, keepdims=True) + 1e-6)


LEAD, GAP, AHEAD, DY = 0, 0, 5, 6


def place(n):
    side = math.isqrt(n)
    me = lax.axis_index("dp")
    x, y = me // side, lax.rem(me, side)

    def at(v, u, w):
        u, w = lax.rem(u + 2 * side, side), lax.rem(w + 2 * side, side)
        return u * side + w if v == 0 else w * side + u

    return me, side, ((x, y), (y, x)), at


def regroup(pieces, lane):
    for k in range(PER):
        out = pieces[k]
        for q in range(PER):
            if q != k:
                out = jnp.where(lane == q, pltpu.roll(pieces[q], (PIECE * (q - k)) % LANES, 1), out)
        yield k, out


def kernel(
    n, x_in, dy_in, wg_in, wu_in, wd_in, dx_out, dwg_out, dwu_out, dwd_out, g_ref,
    local, own, x_ref, h_ref, a_ref, at_ref, d_ref, shared, hid_ref, dg_ref, du_ref, dag, dau, w_buf, terms, mixed, result, result_down,
    sum_p, sum_q, swap_s, swap_r, raw_p_s, raw_p_r, run_p_s, run_p_r, raw_q_s, raw_q_r, run_q_s, run_q_r, turn_s, turn_r, last_s, last_r,
    in_sem, local_sem, down_sem, keep_sem, send_sem, recv_sem, pair_send, pair_recv, load_sem, out_sem, share_ss, share_rs,
    swap_ss, swap_rs, raw_p_ss, raw_p_rs, run_p_ss, run_p_rs, raw_q_ss, raw_q_rs, run_q_ss, run_q_rs, turn_ss, turn_rs, last_ss, last_rs,
):
    layers, chunks = g_ref.shape[:2]
    low, width = own.shape[3:]
    height, part = 2 * low, width // 2
    tokens, depth = x_ref.shape
    me, side, uw, at = place(n)
    x, y = uw[0]
    mate = x + 1 - 2 * lax.rem(x, 2)
    twin = lax.rem(x + 2 * lax.rem(x, 2) - 1 + side, side)
    twin_mate = twin + 1 - 2 * lax.rem(twin, 2)
    parity = lax.rem((x + 1) // 2, 2)
    rep = lax.axis_index("rep")
    core = lax.rem(rep, 2)
    partner = rep + 1 - 2 * core
    half = chunks // 2
    units = layers * half
    opening = half + 6 + GAP
    ahead, by_y = AHEAD * half // 8, DY * half // 8
    turnover = LEAD + half

    barrier = pltpu.get_barrier_semaphore()
    for s in SIGNS:
        pl.semaphore_signal(barrier, inc=1, device_id={"dp": at(0, x + s, y)}, device_id_type=MESH)
        pl.semaphore_signal(barrier, inc=1, device_id={"dp": at(0, x, y + s)}, device_id_type=MESH)
    pl.semaphore_signal(barrier, inc=1, device_id={"rep": partner}, device_id_type=MESH)


    first = pl.multiple_of(core * low, low)

    def fetch(layer, m):
        return pltpu.make_async_copy((wg_in, wu_in)[m].at[layer, pl.ds(first, low)], local.at[layer, m], local_sem.at[layer, m])

    def fetch_down(layer):
        return pltpu.make_async_copy(wd_in.at[layer, :, pl.ds(first, low)], own.at[layer, :, 2], down_sem.at[layer])

    inputs = [pltpu.make_async_copy(x_in, x_ref, in_sem.at[0]), pltpu.make_async_copy(dy_in, d_ref.at[pl.ds(0, tokens)], in_sem.at[1])]
    for layer in range(layers):
        for m in range(2):
            fetch(layer, m).start()
        fetch_down(layer).start()
    for copy in inputs:
        copy.start()

    lane_low = lax.broadcasted_iota(jnp.int32, (low, LANES), 1) // PIECE
    lane_high = lax.broadcasted_iota(jnp.int32, (height, LANES), 1) // PIECE
    per_device = wg_in.shape[2] // n
    tiles, groups = per_device // LANES, n // PER

    def columns(u, q, t):
        return pl.ds(pl.multiple_of((PER * u + q) * per_device + t * LANES, LANES), LANES)

    def tile_of(u):
        return pl.ds(pl.multiple_of(u * LANES, LANES), LANES)

    def keep(i):
        layer, some = i // tiles, pl.ds(PER * lax.rem(i, tiles), PER)
        return pltpu.make_async_copy(own.at[layer, some], g_ref.at[layer, some, me, core], keep_sem.at[i])

    def fill(i):
        layer, t = i // tiles, lax.rem(i, tiles)

        @pl.when(t == 0)
        def _():
            for m in range(2):
                fetch(layer, m).wait()
            fetch_down(layer).wait()

        def once(u, _):
            for m in range(2):
                pieces = [local[layer, m, :, columns(u, q, t)].astype(F32) for q in range(PER)]
                for k, out in regroup(pieces, lane_low):
                    own[layer, PER * t + k, m, :, tile_of(u)] = out.astype(BF16)
            return 0

        lax.fori_loop(0, groups, once, 0)
        keep(i).start()


    def place_of(k, v):
        return k // half, 2 * lax.rem(k, half) + v

    def block(k, v, d):
        layer, j = place_of(k, v)
        return g_ref.at[layer, j, d, core]

    def copy_to(k, v, d, device, src=None):
        return pltpu.make_async_remote_copy(
            src_ref=block(k, v, d) if src is None else src,
            dst_ref=block(k, v, d),
            send_sem=send_sem,
            recv_sem=recv_sem.at[k, v, d],
            device_id={"dp": device},
            device_id_type=MESH,
        )

    def await_block(k, v, d):
        copy_to(k, v, d, me).wait_recv()

    def begin(k):
        for v, (u, w) in enumerate(uw):
            layer, j = place_of(k, v)
            for s in SIGNS:
                copy_to(k, v, me, at(v, u + s, w), own.at[layer, j]).start()
                copy_to(k, v, me, at(v, u, w + s), own.at[layer, j]).start()

    def spread(k, v, d, u, w):
        for s in SIGNS:
            copy_to(k, v, d, at(v, u, w + s)).start()

    def pass_on(k, v, column, sign):
        u, w = uw[v]
        for s in SIGNS:
            await_block(k, v, at(v, u + column, w + s))
        copy_to(k, v, at(v, u + column, w - sign), at(v, u, w + sign)).start()

    def ways(k):
        sign, later = 1 - 2 * lax.rem(k, 2), k // (half + 3 * half // 4)
        across = (2 * lax.rem(x, 2) - 1) * (1 - 2 * later)
        first = 1 - (k + units - half // 2) // units
        return across, sign, sign + (across - sign) * (later + first), -sign

    def near(k):
        signs = ways(k)
        for v, (u, w) in enumerate(uw):
            for s in SIGNS:
                await_block(k, v, at(v, u + s, w))
            copy_to(k, v, at(v, u - signs[v], w), at(v, u + signs[v], w)).start()
            for s in SIGNS:
                spread(k, v, at(v, u + s, w), u, w)
            pass_on(k, v, 0, signs[1 - v])

    def middle(k):
        signs = ways(k)
        for v, (u, w) in enumerate(uw):
            await_block(k, v, at(v, u + 2, w))
            spread(k, v, at(v, u + 2, w), u, w)
            pass_on(k, v, 1, signs[3 - v])
            pass_on(k, v, -1, signs[1 - v])

    def far(k):
        signs = ways(k)
        for v, (u, w) in enumerate(uw):
            pass_on(k, v, 2, signs[3 - v])
            await_block(k, v, at(v, u, w + 2))

    def pair_copy(k, whose):
        layer, j = place_of(k, 0)
        ref = g_ref.at[layer, pl.ds(j, 2), :, whose]
        return pltpu.make_async_remote_copy(
            src_ref=ref, dst_ref=ref, send_sem=pair_send, recv_sem=pair_recv.at[k], device_id={"rep": partner}, device_id_type=MESH
        )

    def last(k):
        for v, (u, w) in enumerate(uw):
            for column in (1, -1, 2):
                await_block(k, v, at(v, u + column, w + 2))

        @pl.when(lax.rem(k, PER // 2) == 0)
        def _():
            keep(k // (PER // 2)).wait()

        pair_copy(k, core).start()


    def load(layer, j, slot):
        return pltpu.make_async_copy(g_ref.at[layer, j], w_buf.at[slot], load_sem.at[slot])

    def load_unit(k, v):
        return load(0, 2 * k + v, 2 * lax.rem(k, 2) + v)

    def load_other(o):
        return load(layers - 1 - o // half, 2 * lax.rem(o, half) + 1 - parity, lax.rem(o, 2))

    def load_mine(c):
        return load(layers - 1 - c // half, 2 * lax.rem(c, half) + parity, 2 + lax.rem(c, 2))

    def both(k):
        pair_copy(k, 1 - core).wait_recv()

        @pl.when(k < half)
        def _():
            for v in range(2):
                load_unit(k, v).start()

    mine_rows, mate_rows = pl.ds(0, tokens), pl.ds(tokens, tokens)

    def matrices(slot):
        return [w_buf[slot, :, :, m].reshape(depth, width) for m in range(3)]

    def sigmoid(z):
        return 0.5 * jnp.tanh(0.5 * z) + 0.5

    def forward(k, rows, total):
        for v in range(2):
            if rows is mine_rows:
                load_unit(k, v).wait()
            wg, wu, wd = matrices(2 * lax.rem(k, 2) + v)
            a = a_ref[rows]
            gate, up = dot(a, wg), dot(a, wu)
            total[...] += dot((gate * sigmoid(gate) * up).astype(BF16), wd)


    def share(kind, piece, count=1):
        rows = pl.ds(piece * (tokens // half), count * (tokens // half))
        source = (x_ref, h_ref, d_ref, d_ref)[kind]
        return pltpu.make_async_remote_copy(
            src_ref=source.at[rows],
            dst_ref=shared.at[kind, rows],
            send_sem=share_ss.at[kind],
            recv_sem=share_rs.at[kind],
            device_id={"dp": at(0, mate, y)},
            device_id_type=MESH,
        )

    def share_all(kind):
        return share(kind, 0, half)


    def normed(source, rows):
        wide = source.astype(F32)
        a = wide * scale_of(wide)
        a_ref[rows] = a.astype(BF16)
        at_ref[:, rows] = a.T.astype(BF16)

    def start_layer(source):
        normed(source[...], mine_rows)
        dag[...] = jnp.zeros_like(dag)

    def meet(kind, by_kind):
        normed(shared[kind], mate_rows)
        share_all(by_kind).wait_recv()
        d_ref[mate_rows] = shared[by_kind]

    def end_layer(source):
        wide = source[...].astype(F32)
        scale = scale_of(wide)
        da = (dag[...].astype(BF16) + dau[...].astype(BF16)).astype(F32)
        inner = jnp.sum(da * wide, -1, keepdims=True)
        by_h = da * scale - wide * (scale * scale * scale * inner / depth)
        d_ref[mine_rows] = d_ref[mine_rows] + by_h.astype(BF16)

    def by_hidden(slot, rows, kept):
        wg, wu, wd = matrices(slot)
        a, d = a_ref[rows], d_ref[rows]
        gate, up = dot(a, wg), dot(a, wu)
        by_hid = dot(d, wd, NT).astype(BF16).astype(F32)
        sig = sigmoid(gate)
        silu = gate * sig
        dg = (by_hid * up * (sig + silu * (1 - sig))).astype(BF16)
        du = (by_hid * silu).astype(BF16)
        if kept:
            hid_ref[rows] = (silu * up).astype(BF16)
            dg_ref[rows] = dg
            du_ref[rows] = du
        return dg, du, wg, wu

    def own_part(slot, kept):
        dg, du, wg, wu = by_hidden(slot, mine_rows, kept)
        dag[...] += dot(dg, wg, NT)
        dau[...] += dot(du, wu, NT)

    def compute(c):
        held, slot = lax.rem(c, 3), 2 + lax.rem(c, 2)
        load_mine(c).wait()
        own_part(slot, True)
        by_hidden(slot, mate_rows, True)
        step = n
        for m, (left, right, dims) in enumerate(((at_ref, dg_ref, NN), (at_ref, du_ref, NN), (hid_ref, d_ref, TN))):
            for i in range(1):
                some = pl.ds(i * step * height, step * height)
                value = dot(left[some] if dims is NN else left[:, some], right[...], dims)
                terms[held, m, i * step : (i + 1) * step] = value.reshape(step, height, width)


    P_ROWS, Q_ROWS = slice(0, low), slice(low, height)
    MINE, THEIRS = (x, mate), (twin, twin_mate)

    def cols_of(h):
        return slice(h * part, (h + 1) * part)

    def remote(k, src, dst, src_sem, dst_sem, device, *index):
        return pltpu.make_async_remote_copy(
            src_ref=src.at[(lax.rem(k, 2), *index)],
            dst_ref=dst.at[(lax.rem(k, 4), *index)],
            send_sem=src_sem.at[(lax.rem(k, 2), *index)],
            recv_sem=dst_sem.at[(lax.rem(k, 4), *index)],
            device_id={"dp": device},
            device_id_type=MESH,
        )

    def down_the_column(src, dst, src_sem, dst_sem):
        return lambda k: [remote(k, src, dst, src_sem, dst_sem, at(0, x, y + s), i) for i, s in enumerate(SIGNS)]

    swap = lambda k: [remote(k, swap_s, swap_r, swap_ss, swap_rs, at(0, twin, y))]
    turn = lambda k: [remote(k, turn_s, turn_r, turn_ss, turn_rs, at(0, twin, y))]
    hand = lambda k: [remote(k, last_s, last_r, last_ss, last_rs, at(0, mate, y))]
    raw_p = down_the_column(raw_p_s, raw_p_r, raw_p_ss, raw_p_rs)
    run_p = down_the_column(run_p_s, run_p_r, run_p_ss, run_p_rs)
    raw_q = down_the_column(raw_q_s, raw_q_r, raw_q_ss, raw_q_rs)
    run_q = down_the_column(run_q_s, run_q_r, run_q_ss, run_q_rs)

    def go(copies):
        for copy in copies:
            copy.start()

    def arrive(copies):
        for copy in copies:
            copy.wait()

    def row(w):
        return lax.rem(w + 2 * side, side)

    def slots(k):
        return lax.rem(k, 3), lax.rem(k, 2), lax.rem(k, 4)

    def pack(c):
        held, slot, _ = slots(c)
        for e, column in enumerate(THEIRS):
            for w in range(side):
                swap_s[slot, e, w] = terms[held, :, at(0, column, w), P_ROWS].astype(BF16)
        go(swap(c))
        for i, s in enumerate(SIGNS):
            for u in range(side):
                raw_q_s[slot, i, 0, u] = terms[held, :, at(0, u, y + 2), Q_ROWS, cols_of(i)].astype(BF16)
                raw_q_s[slot, i, 1, u] = terms[held, :, at(0, u, y + s), Q_ROWS, cols_of(1 - i)].astype(BF16)
        go(raw_q(c))

    def stage1(c):
        held, slot, got = slots(c)
        arrive(swap(c))
        for e, column in enumerate(MINE):
            for w in range(side):
                sum_p[slot, e, w] = terms[held, :, at(0, column, w), P_ROWS] + swap_r[got, e, w].astype(F32)
        for i, s in enumerate(SIGNS):
            for e in range(2):
                raw_p_s[slot, i, 0, e] = sum_p[slot, e, row(y + 2), :, :, cols_of(i)].astype(BF16)
                raw_p_s[slot, i, 1, e] = sum_p[slot, e, row(y + s), :, :, cols_of(1 - i)].astype(BF16)
        go(raw_p(c))
        arrive(raw_q(c))
        for i, s in enumerate(SIGNS):
            for u in range(side):
                value = terms[held, :, at(0, u, y + s), Q_ROWS, cols_of(i)] + raw_q_r[got, i, 0, u].astype(F32)
                run_q_s[slot, i, u] = value.astype(BF16)
        go(run_q(c))

    def stage2(c):
        held, slot, got = slots(c)
        arrive(raw_p(c))
        for i, s in enumerate(SIGNS):
            for e in range(2):
                value = sum_p[slot, e, row(y + s), :, :, cols_of(i)] + raw_p_r[got, i, 0, e].astype(F32)
                run_p_s[slot, i, e] = value.astype(BF16)
        go(run_p(c))
        arrive(run_q(c))
        for i in range(2):
            for e in range(2):
                for column, mine in ((MINE[e], True), (THEIRS[e], False)):
                    value = terms[held, :, at(0, column, y), Q_ROWS, cols_of(i)]
                    value = value + run_q_r[got, i, column].astype(F32) + raw_q_r[got, 1 - i, 1, column].astype(F32)
                    if mine:
                        sum_q[slot, e, :, :, cols_of(i)] = value
                    else:
                        turn_s[slot, e, :, :, cols_of(i)] = value.astype(BF16)
        go(turn(c))

    def own_chunk(c, other):
        return layers - 1 - c // half, 2 * lax.rem(c, half) + (1 - parity if other else parity)

    def settle(c, value, rows, cols):
        layer, j = own_chunk(c, False)
        mixed[:, lax.rem(j, PER), rows, cols] = value[:2]
        result_down[layer, j, rows, cols] = value[2]

    def stage3(c):
        held, slot, got = slots(c)
        arrive(run_p(c))
        for i in range(2):
            for e in range(2):
                value = sum_p[slot, e, y, :, :, cols_of(i)] + run_p_r[got, i, e].astype(F32) + raw_p_r[got, 1 - i, 1, e].astype(F32)
                if e == 0:
                    settle(c, value.astype(BF16), P_ROWS, cols_of(i))
                else:
                    last_s[slot, :, P_ROWS, cols_of(i)] = value.astype(BF16)
        arrive(turn(c))
        for e in range(2):
            value = (sum_q[slot, e] + turn_r[got, e].astype(F32)).astype(BF16)
            if e == 0:
                settle(c, value, Q_ROWS, slice(0, width))
            else:
                last_s[slot, :, Q_ROWS] = value
        go(hand(c))

    def put(layer):
        return [
            pltpu.make_async_copy(src.at[layer], dst.at[layer], out_sem.at[layer, m])
            for m, (src, dst) in enumerate(((result.at[0], dwg_out), (result.at[1], dwu_out), (result_down, dwd_out)))
        ]

    def stage4(c):
        _, _, got = slots(c)
        layer, j = own_chunk(c, True)
        arrive(hand(c))
        mixed[:, lax.rem(j, PER)] = last_r[got, :2]
        result_down[layer, j] = last_r[got, 2]

        @pl.when(lax.rem(c, PER // 2) == PER // 2 - 1)
        def _():
            def once(u, _):
                for m in range(2):
                    pieces = [mixed[m, q, :, tile_of(u)].astype(F32) for q in range(PER)]
                    for q, out in regroup(pieces, lane_high):
                        result[m, layer, :, columns(u, q, j // PER)] = out.astype(BF16)
                return 0

            lax.fori_loop(0, groups, once, 0)

        @pl.when(lax.rem(c, half) == half - 1)
        def _():
            for copy in put(layer):
                copy.start()

    def unit_at(t):
        q = t // (half + GAP)
        return t - GAP * q, (t >= 0) & (t < 2 * half + GAP) & (t - q * (half + GAP) < half)

    def mine_at(r):
        r = r - LEAD
        q = (r + 1024 - half - ahead) // 1024
        c = r - q * ahead
        return c, (r >= 0) & (r - q * (half + ahead) < half), (r >= 0) & ((r < half) | (q == 1))

    def other_at(r):
        late = r - turnover
        q = late // (half + ahead)
        return (r, (r >= 0) & (r < half)), (half + late - q * half, ((late >= 0) & (late < ahead)) | ((late >= half + ahead) & (late < 2 * half)))

    fill(0)
    pl.semaphore_wait(barrier, 5)

    def stages_at(t, *stages):
        for lag, stage in stages:
            k, here = unit_at(t - lag)

            @pl.when((t >= lag) & here)
            def _(k=k, stage=stage):
                stage(k)

    def step(t, _):
        r = t - opening
        (o, early), (o_late, late) = other_at(r)
        (o_soon, soon), (o_next, next_late) = other_at(r + 1)
        c, mine, going = mine_at(r)
        c_next, mine_next, _ = mine_at(r + 1)

        @pl.when(r == turnover)
        def _():
            share_all(2).wait_send()
            end_layer(h_ref)
            share_all(3).start()
            start_layer(x_ref)
            dau[...] = jnp.zeros_like(dau)

        @pl.when(mine_next & (c_next >= half))
        def _():
            load_mine(c_next).start()

        for lag, stage in ((5, stage4), (4, stage3), (3, stage2), (2, stage1)):

            @pl.when(going & (c >= lag) & (c - lag < 2 * half))
            def _(lag=lag, stage=stage):
                stage(c - lag)

        @pl.when(next_late)
        def _():
            load_other(o_next).start()

        @pl.when(early | late)
        def _():
            chunk = o - (o - o_late) * ((r + 2 * half) // (turnover + 2 * half))
            load_other(chunk).wait()
            own_part(lax.rem(chunk, 2), False)

        stages_at(t, (5, both), (0, begin), (1, near), (2, middle), (3, far), (4, last))

        @pl.when(mine_next & (c_next < half) & (c_next > 0))
        def _():
            load_mine(c_next).start()

        @pl.when(soon)
        def _():
            load_other(o_soon).start()

        coming, here = unit_at(t + 1)

        @pl.when(here & (lax.rem(coming, PER // 2) == 0))
        def _():
            fill(coming // (PER // 2))

        @pl.when(t == 0)
        def _():
            for copy in inputs:
                copy.wait()
            wide = x_ref[...].astype(F32)
            a_ref[mine_rows] = (wide * scale_of(wide)).astype(BF16)
            dag[...] = jnp.zeros_like(dag)
            dau[...] = jnp.zeros_like(dau)

        @pl.when((t < 6) & (t + t // 3 < half))
        def _():
            share(0, t + t // 3).start()

        @pl.when((lax.rem(t, 3) == 2) & (t + t // 3 + 1 < half))
        def _():
            share(0, t + t // 3 + 1).start()

        @pl.when((t >= by_y) & (t < by_y + half))
        def _():
            share(2, t - by_y).start()

        @pl.when((t >= 5) & (t < half + 5))
        def _():
            forward(t - 5, mine_rows, dag)

        @pl.when(t == 6)
        def _():
            share_all(0).wait_recv()
            wide = shared[0].astype(F32)
            a_ref[mate_rows] = (wide * scale_of(wide)).astype(BF16)

        @pl.when((t >= 6) & (t < half + 6))
        def _():
            forward(t - 6, mate_rows, dau)

        @pl.when(t == half + 4)
        def _():
            h_ref[...] = x_ref[...] + dag[...].astype(BF16)
            start_layer(h_ref)

        @pl.when(t == half + 5)
        def _():
            shared[1] = shared[0] + dau[...].astype(BF16)
            dau[...] = jnp.zeros_like(dau)
            load_mine(0).start()

        @pl.when(r == LEAD)
        def _():
            meet(1, 2)

        @pl.when(r == turnover + ahead)
        def _():
            meet(0, 3)

        @pl.when((r >= LEAD) & mine)
        def _():
            compute(c)
            pack(c)

        @pl.when(r == turnover + 2 * half)
        def _():
            share_all(3).wait_send()
            end_layer(x_ref)
            pltpu.make_async_copy(d_ref.at[mine_rows], dx_out, in_sem.at[0]).start()

        return 0

    lax.fori_loop(0, opening + turnover + max(2 * half + 1, ahead + half + 5), step, 0)
    share_all(0).wait_send()
    pltpu.make_async_copy(d_ref.at[mine_rows], dx_out, in_sem.at[0]).wait()
    for layer in range(layers):
        for copy in put(layer):
            copy.wait()
    for sem, blocks in ((send_sem, n - 1), (pair_send, n)):
        ref = g_ref.at[:, :, pl.ds(0, blocks), 0]
        pltpu.make_async_copy(ref, ref, sem).wait()


def copy_kernel(*refs):
    count = (len(refs) - 2) // 3
    given, got, held, (in_sem, out_sem) = refs[:count], refs[count : 2 * count], refs[2 * count : 3 * count], refs[3 * count :]
    come = [pltpu.make_async_copy(a, b, in_sem.at[i]) for i, (a, b) in enumerate(zip(given, held, strict=True))]
    leave = [pltpu.make_async_copy(a, b, out_sem.at[i]) for i, (a, b) in enumerate(zip(held, got, strict=True))]
    for copy in come:
        copy.start()
    for first, second in zip(come, leave, strict=True):
        first.wait()
        second.start()
    for copy in leave:
        copy.wait()


def copied(*arrays):
    anywhere = pl.BlockSpec(memory_space=pl.ANY)
    return pl.pallas_call(
        copy_kernel,
        out_shape=[jax.ShapeDtypeStruct(a.shape, a.dtype) for a in arrays],
        in_specs=[anywhere] * len(arrays),
        out_specs=[anywhere] * len(arrays),
        scratch_shapes=[*[pltpu.VMEM(a.shape, a.dtype) for a in arrays], *[pltpu.SemaphoreType.DMA((len(arrays),))] * 2],
        compiler_params=pltpu.CompilerParams(vmem_limit_bytes=VMEM_LIMIT),
        name="copied",
    )(*arrays)


def run(n, x, dy, wg, wu, wd):
    (layers, height, local_width), (tokens, depth) = wg.shape, x.shape
    width = n * PIECE
    chunks = wd.shape[1] // PIECE
    assert depth == width and height == PIECE and layers == 2
    low, side, part = height // 2, math.isqrt(n), width // 2
    anywhere = pl.BlockSpec(memory_space=pl.ANY)
    sems = lambda *counts: pltpu.SemaphoreType.DMA(counts)
    bf16, f32 = (lambda *dims: pltpu.VMEM(dims, BF16)), (lambda *dims: pltpu.VMEM(dims, F32))
    whole, block = (3, low, width), (3, low, part)
    piece = (n, 2, 3, low, width)
    shape = lambda *dims: jax.ShapeDtypeStruct(dims, BF16)
    down = (layers, chunks, PIECE, depth)
    slots = lambda *dims: [bf16(2, *dims), bf16(4, *dims)]
    *results, _ = pl.pallas_call(
        functools.partial(kernel, n),
        out_shape=(shape(*x.shape), shape(*wg.shape), shape(*wu.shape), shape(*down), shape(layers, chunks, *piece)),
        in_specs=[anywhere] * 5,
        out_specs=(anywhere,) * 5,
        scratch_shapes=[
            bf16(layers, 2, low, local_width),
            bf16(layers, chunks, *whole),
            *[bf16(*x.shape)] * 2,
            bf16(2 * tokens, depth), bf16(depth, 2 * tokens), bf16(2 * tokens, depth),
            bf16(4, tokens, depth),
            *[bf16(2 * tokens, width)] * 3,
            *[f32(*x.shape)] * 2,
            bf16(4, *piece),
            f32(3, 3, n, height, width),
            bf16(2, PER, height, width), bf16(2, *wg.shape), bf16(*down),
            f32(2, 2, side, *whole), f32(2, 2, *whole),
            *slots(2, side, *whole),
            *slots(2, 2, 2, *block), *slots(2, 2, *block),
            *slots(2, 2, side, *block), *slots(2, side, *block),
            *slots(2, *whole), *slots(3, height, width),
            sems(2), sems(layers, 2), sems(layers), sems(layers * chunks // PER),
            pltpu.SemaphoreType.DMA, sems(layers * chunks // 2, 2, n), pltpu.SemaphoreType.DMA, sems(layers * chunks // 2),
            sems(4), sems(layers, 3), sems(4), sems(4),
            sems(2), sems(4), *[sems(2, 2), sems(4, 2)] * 4, *[sems(2), sems(4)] * 2,
        ],
        compiler_params=pltpu.CompilerParams(collective_id=0, has_side_effects=True, vmem_limit_bytes=VMEM_LIMIT),
        name="layers",
    )(x, dy, wg, wu, wd.reshape(down))
    dx, dwg, dwu, dwd = copied(*results)
    return dx, dwg, dwu, dwd.reshape(wd.shape)


def solution(mesh):
    n = mesh.shape["dp"]

    def step(x, dy, wg, wu, wd):
        dx, *by_weights = run(n, x[0], dy[0], wg, wu, wd)
        return (dx[None], *by_weights)

    tokens, rows, out = P(("rep", "dp"), None, None), P(None, "dp", None), P("rep", "dp", None)
    return jax.shard_map(step, mesh=mesh, in_specs=(tokens, tokens, rows, rows, rows), out_specs=(tokens, out, out, out), check_vma=False)
```
